256 devices in a mesh: sub: 4 (over x), row: 4 (over y_lo, core), col: 16 (over z, y_hi).
Axes of the slice: x: 4, y: 4 (y_hi: 2, y_lo: 2; y = y_hi * 2 + y_lo), z: 8, core: 2. Of those that a mesh axis runs over, the one named last changes fastest.
Arguments:
- leaf_sizes: int32 [512], P(('sub', 'row', 'col')), may hold values from 20 to 219
- remap: int32 [4], replicated, may hold values from 0 to 3, each once
- panel_diag: float32 [4, 1536, 1536], P('sub', ('row', 'col')), may hold values from -1 to 6, as said below
- panel_below: float32 [4, 5632, 1536], P('sub', ('row', 'col')), may hold values from -1.2 to 1.2
- trailing: float32 [4, 5632, 5632], P('sub', 'row', 'col'), may hold values from -6 to 26, as said below
Outputs:
- diag_factor: float32 [4, 1536, 1536], P('sub', ('row', 'col'))
- panel_factor: float32 [4, 5632, 1536], P('sub', ('row', 'col'))
- schur: float32 [4, 5632, 5632], P('sub', 'row', 'col')
- subtree_cost: float32 [4], P('sub')
The draws below stay inside these ranges and needn't reach their ends.
Inputs may be any that keep to these rules, and one draw needn't show every extreme that they name: remap is a permutation: front j moves to subcube remap[j]. `panel_diag`: each front's block is symmetric and positive definite. `trailing`: each front's block is symmetric.
All inputs are finite; a program needn't handle non-finite values.
Results may differ from the reference program's by a relative error of at most 0.0001.
Values sent between devices are 32-bit elements; how exact they have to be, the bound alone decides.
No kernel may reach another device: no remote copies, remote signals or barrier semaphores. Data moves between devices by JAX's collectives and lax.ppermute only.
A program may use at most 128 MiB of HBM per device.

```python
import jax
import jax.numpy as jnp
from jax import lax

P_SIZE = 1536
R = 5632
NF = 4
SUB_LEAVES = 128
LEAVES = 512


def symmetric_noise(key, count, order):
    noise = jnp.clip(jax.random.normal(key, (count, order, order), jnp.float32), -4.0, 4.0)
    return (noise + jnp.swapaxes(noise, 1, 2)) * 0.7071


def draw_panel_diag(key, part):
    noise_key, diag_key = jax.random.split(jax.random.fold_in(key, 11))
    sym_part = symmetric_noise(noise_key, NF, P_SIZE) * P_SIZE ** (-0.5)
    diagonal = jax.random.uniform(diag_key, (NF, P_SIZE), jnp.float32, 3.0, 5.0)
    return sym_part + diagonal[:, :, None] * jnp.eye(P_SIZE, dtype=jnp.float32)[None, :, :]


def draw_trailing(key, part):
    noise_key, diag_key = jax.random.split(jax.random.fold_in(key, 23))
    sym_part = symmetric_noise(noise_key, NF, R)
    diagonal = jax.random.uniform(diag_key, (NF, R), jnp.float32, 16.0, 20.0)
    return sym_part + diagonal[:, :, None] * jnp.eye(R, dtype=jnp.float32)[None, :, :]


def set_ends(drawn, rng, smallest, largest):
    index_at = [jax.random.randint(jax.random.fold_in(rng, axis), (), 0, length) for axis, length in enumerate(drawn.shape)]
    widest = drawn.shape.index(max(drawn.shape))
    neighbour = index_at[:widest] + [(index_at[widest] + 1) % drawn.shape[widest]] + index_at[widest + 1:]
    return drawn.at[tuple(index_at)].set(smallest).at[tuple(neighbour)].set(largest)


def block_levels(rng, dims, cuts, smallest, top_value):
    factor_of = 1.0
    for dim, parts in cuts:
        heights = jax.random.uniform(jax.random.fold_in(jax.random.fold_in(rng, 6), dim), (parts,), jnp.float32, smallest / len(cuts), top_value / len(cuts))
        factor_of = factor_of * jnp.repeat(jnp.exp(heights), dims[dim] // parts).reshape((-1,) + (1,) * (len(dims) - 1 - dim))
    return factor_of


def scatter_about(key, dims, scale, most, cuts=(), kind=jnp.bfloat16):
    drawn = scale * jax.random.normal(key, dims, jnp.float32)
    if cuts:
        drawn = drawn * block_levels(key, dims, cuts, -0.22, 0.18)
    return jnp.clip(drawn, -most, most).astype(kind)


def setup_inputs(seed: int = 0) -> dict:
    key_of = jax.random.split(jax.random.key(seed), 6)
    leaf_sizes = set_ends(jax.random.randint(key_of[0], (LEAVES,), 20, 220), jax.random.fold_in(key_of[0], 1), 20, 219).astype(jnp.int32)
    remap = jax.random.permutation(key_of[1], NF).astype(jnp.int32)
    panel_diag = draw_panel_diag(jax.random.fold_in(key_of[5], 71), 0)
    panel_below = scatter_about(key_of[3], (NF, R, P_SIZE), 0.2, 1.2, ((0, 4), (1, 64)), jnp.float32)
    trailing = draw_trailing(jax.random.fold_in(key_of[5], 71), 0)
    return dict(leaf_sizes=leaf_sizes, remap=remap, panel_diag=panel_diag, panel_below=panel_below, trailing=trailing)


def reference(leaf_sizes, remap, panel_diag, panel_below, trailing):
    scaled = leaf_sizes.astype(jnp.float32) / 100.0
    cubes = jnp.reshape(scaled * scaled * scaled, (NF, SUB_LEAVES))
    subtree_cost = jnp.sum(cubes, axis=1) / SUB_LEAVES
    factors = []
    panels = []
    schurs = []
    for target in range(NF):
        source = jnp.sum(jnp.arange(NF, dtype=jnp.int32) * (remap == target).astype(jnp.int32))
        diag_block = lax.dynamic_index_in_dim(panel_diag, source, 0, keepdims=False)
        below_block = lax.dynamic_index_in_dim(panel_below, source, 0, keepdims=False)
        trail_block = lax.dynamic_index_in_dim(trailing, source, 0, keepdims=False)
        factor_low = jnp.linalg.cholesky(diag_block)
        solved = lax.linalg.triangular_solve(factor_low, below_block, left_side=False, lower=True, transpose_a=True)
        update = lax.dot_general(solved.astype(jnp.float32), solved.astype(jnp.float32), (((1,), (1,)), ((), ())), precision=lax.Precision.HIGHEST, preferred_element_type=jnp.float32)
        factors.append(factor_low)
        panels.append(solved)
        schurs.append(trail_block - update)
    return (jnp.stack(factors), jnp.stack(panels), jnp.stack(schurs), subtree_cost)
```

```python
import jax
import jax.numpy as jnp
from jax import lax
from jax.experimental import pallas as pl
from jax.experimental.pallas import tpu as pltpu
from jax.sharding import Mesh
from jax.sharding import PartitionSpec as P

ROW = ("row_0", "row_1")
COL = ("col_0", "col_1")
ROW_COL = ("row_0", "row_1", "col_0", "col_1")
SUB_ROW_COL = ("sub", "row_0", "row_1", "col_0", "col_1")

HI = lax.Precision.HIGHEST


def nt(a, b):
    return lax.dot_general(a, b, (((1,), (1,)), ((), ())), precision=HI, preferred_element_type=jnp.float32)


def nn(a, b):
    return lax.dot_general(a, b, (((1,), (0,)), ((), ())), precision=HI, preferred_element_type=jnp.float32)


def over_lanes(x, lane):
    return jnp.broadcast_to(x[:, lane:lane + 1], x.shape)


def over_sublanes(x, row):
    return jnp.broadcast_to(x[row:row + 1, :], x.shape)


def factor_block(block_ref, inverse_ref, upper_ref):
    size = block_ref.shape[0]
    groups = size // 8
    lanes = lax.broadcasted_iota(jnp.int32, (8, size), 1)
    subs = lax.broadcasted_iota(jnp.int32, (8, size), 0)
    rows = [block_ref[8 * q:8 * q + 8, :] for q in range(groups)]
    for p in range(groups):
        inside = (lanes >= 8 * p) & (lanes < 8 * p + 8)
        plain = rows[p]
        unit = jnp.where(inside, jnp.where(lanes == subs + 8 * p, 1.0, 0.0), plain)
        cols = [over_lanes(plain, 8 * p + l) for l in range(8)]
        below = {q: [over_lanes(rows[q], 8 * p + l) for l in range(8)] for q in range(p + 1, groups)}
        pivots = jnp.ones_like(plain)
        for j in range(8):
            u = {l: over_sublanes(cols[l], j) for l in range(j, 8)}
            pivots = jnp.where(subs == j, u[j], pivots)
            inv = 1.0 / u[j]
            coef = cols[j] * inv
            for l in range(j + 1, 8):
                cols[l] = cols[l] - coef * u[l]
            masked = jnp.where(subs > j, coef, 0.0)
            plain = plain - masked * over_sublanes(plain, j)
            unit = unit - masked * over_sublanes(unit, j)
            for q in below:
                v = below[q]
                v[j] = v[j] * inv
                for l in range(j + 1, 8):
                    v[l] = v[l] - v[j] * u[l]
        spread = [over_sublanes(unit, j) for j in range(8)]
        for q in below:
            v = below[q]
            t = [v[j] * spread[j] for j in range(8)]
            s = ((t[0] + t[1]) + (t[2] + t[3])) + ((t[4] + t[5]) + (t[6] + t[7]))
            rows[q] = jnp.where(inside, 0.0, rows[q]) - s
        scale = lax.rsqrt(pivots)
        upper_ref[8 * p:8 * p + 8, :] = jnp.where(lanes >= subs + 8 * p, plain * scale, 0.0)
        inverse_ref[8 * p:8 * p + 8, :] = jnp.where(lanes <= subs + 8 * p, unit * scale, 0.0)


NB = 128
WB = 256


def panel_kernel(where_ref, mine_ref, other_ref, below_ref, c0_ref, c1_ref, c2_ref, c3_ref,
                 diag_out, own_out, y_out, cost_out, work, block, inverse, upper, pair, sems):
    n = work.shape[1]
    blocks = n // WB
    total = work.shape[0] // WB
    y_at, core, row_at, flat = where_ref[0], where_ref[1], where_ref[2], where_ref[3]
    z_count, s_count, piece_rows, _ = mine_ref.shape
    copies = []
    for side, ref in ((0, mine_ref), (1, other_ref)):
        core_of = lax.rem(core + side, 2)
        for s in range(s_count):
            y_of = lax.rem(y_at + s, 4)
            base = (lax.rem(y_of, 2) * 2 + core_of) * 2 * z_count + lax.div(y_of, 2)
            for z in range(z_count):
                at = pl.multiple_of((base + 2 * z) * piece_rows, 8)
                copies.append((ref.at[z, s], work.at[pl.ds(at, piece_rows), :]))
    own_rows = below_ref.shape[0]
    for s, ref in enumerate((c0_ref, c1_ref, c2_ref, c3_ref)):
        at = pl.multiple_of(n + lax.rem(row_at - s + 4, 4) * own_rows, 8)
        copies.append((ref, work.at[pl.ds(at, own_rows), :]))
    copies.append((below_ref, work.at[pl.ds(n + 4 * own_rows, own_rows), :]))
    copies = [pltpu.make_async_copy(src, dst, sems.at[i]) for i, (src, dst) in enumerate(copies)]
    for c in copies:
        c.start()
    used = n + 5 * own_rows
    work[used:, :] = jnp.zeros((work.shape[0] - used, n), jnp.float32)
    for c in copies:
        c.wait()
    last = slice(n - NB, n)
    corner = work[0:8, last]
    for f in range(1, n // piece_rows):
        corner = corner + work[f * piece_rows:f * piece_rows + 8, last]
    cost_out[...] = corner
    first = (lax.broadcasted_iota(jnp.int32, (8, NB), 0) == 0) & (lax.broadcasted_iota(jnp.int32, (8, NB), 1) == NB - 1)
    for f in range(-(-(n - NB) // piece_rows), n // piece_rows):
        r = f * piece_rows
        mirror = jnp.broadcast_to(work[n - 1:n, r:r + 1], (8, NB))
        work[r:r + 8, last] = jnp.where(first, mirror, work[r:r + 8, last])
    block[...] = work[0:NB, 0:NB]

    def step(j, carry):
        factor_block(block, inverse, upper)
        for jj in range(n // NB):
            @pl.when(j == jj)
            def _(jj=jj):
                J, half = jj // 2, jj % 2
                lo = jj * NB
                if half == 0:
                    work[lo:lo + NB, lo:lo + NB] = upper[...].T
                    low = nt(work[lo + NB:lo + 2 * NB, lo:lo + NB], inverse[...])
                    work[lo + NB:lo + 2 * NB, lo:lo + NB] = low
                    block[...] = work[lo + NB:lo + 2 * NB, lo + NB:lo + 2 * NB] - nt(low, low)
                    pair[J, 0:NB, 0:NB] = inverse[...]
                    pair[J, 0:NB, NB:] = jnp.zeros((NB, NB), jnp.float32)
                else:
                    work[lo:lo + NB, lo:lo + NB] = upper[...].T
                    low = work[lo:lo + NB, lo - NB:lo]
                    pair[J, NB:, 0:NB] = -nn(inverse[...], nn(low, pair[J, 0:NB, 0:NB]))
                    pair[J, NB:, NB:] = inverse[...]
                    both = slice(J * WB, (J + 1) * WB)
                    after = slice((J + 1) * WB, (J + 2) * WB)

                    def solve(i, c):
                        at = pl.ds(pl.multiple_of(i * WB, WB), WB)
                        work[at, both] = nt(work[at, both], pair[J])
                        return c

                    lax.fori_loop(J + 1, total, solve, 0)
                    if J + 1 < blocks:
                        def update(i, c):
                            at = pl.ds(pl.multiple_of(i * WB, WB), WB)
                            work[at, after] = work[at, after] - nt(work[at, :(J + 1) * WB], work[after, :(J + 1) * WB])
                            return c

                        lax.fori_loop(J + 1, total, update, 0)
                        block[...] = work[lo + NB:lo + 2 * NB, lo + NB:lo + 2 * NB]
        return carry

    lax.fori_loop(0, n // NB, step, 0)
    count = diag_out.shape[0]
    at = pl.multiple_of(flat * count, 8)
    found = work[pl.ds(at, count), :]
    r = lax.broadcasted_iota(jnp.int32, found.shape, 0) + flat * count
    c = lax.broadcasted_iota(jnp.int32, found.shape, 1)
    diag_out[...] = jnp.where(c <= r, found, 0.0)
    own_out[...] = work[n + 4 * own_rows:n + 5 * own_rows, :]
    rows = slice(n, n + 4 * own_rows)
    for J in range(blocks - 1, -1, -1):
        both = slice(J * WB, (J + 1) * WB)
        part = work[rows, both]
        if J + 1 < blocks:
            part = part - nn(work[rows, (J + 1) * WB:], work[(J + 1) * WB:n, both])
        work[rows, both] = nn(part, pair[J])
    y_out[...] = work[rows, :]


def panel_call(places, mine, other, below, cs):
    n = mine.shape[-1]
    m = below.shape[0]
    height = -(-(n + 5 * m) // WB) * WB
    anyspec = pl.BlockSpec(memory_space=pl.ANY)
    vm = pl.BlockSpec(memory_space=pltpu.VMEM)
    f32 = jnp.float32
    pieces = 2 * mine.shape[0] * mine.shape[1]
    return pl.pallas_call(
        panel_kernel,
        out_shape=(jax.ShapeDtypeStruct((mine.shape[2], n), f32), jax.ShapeDtypeStruct((m, n), f32), jax.ShapeDtypeStruct((4 * m, n), f32), jax.ShapeDtypeStruct((8, NB), f32)),
        in_specs=[pl.BlockSpec(memory_space=pltpu.SMEM)] + [anyspec] * 7,
        out_specs=(vm, vm, vm, vm),
        scratch_shapes=[
            pltpu.VMEM((height, n), f32), pltpu.VMEM((NB, NB), f32), pltpu.VMEM((NB, NB), f32), pltpu.VMEM((NB, NB), f32),
            pltpu.VMEM((n // WB, WB, WB), f32), pltpu.SemaphoreType.DMA((pieces + 5,)),
        ],
        compiler_params=pltpu.CompilerParams(vmem_limit_bytes=48 * 2**20),
        cost_estimate=pl.CostEstimate(flops=100_000_000_000, bytes_accessed=20_000_000, transcendentals=0),
        name="panel",
    )(places, mine, other, below, *cs)


def shifted(value, axes, size, shift):
    return lax.ppermute(value, axes, [((d + shift) % size, d) for d in range(size)])


def around(value, shift):
    at = [(y % 2) * 2 + y // 2 for y in range(4)]
    return lax.ppermute(value, ("row_0", "col_1"), [(at[(y + shift) % 4], at[y]) for y in range(4)])


def chosen(pieces, which):
    out = pieces[0]
    for k in range(1, len(pieces)):
        out = jnp.where(which == k, pieces[k], out)
    return out


def local(leaf_sizes, remap, panel_diag, panel_below, trailing):
    sub, core = lax.axis_index("sub"), lax.axis_index("row_1")
    y_lo, y_hi, z = lax.axis_index("row_0"), lax.axis_index("col_1"), lax.axis_index("col_0")
    fronts = remap.shape[0]
    row_at = y_lo * 2 + core
    flat = lax.axis_index(ROW_COL)
    columns = lax.axis_size(COL)
    source = jnp.sum(jnp.arange(fronts, dtype=jnp.int32) * (remap == sub).astype(jnp.int32))
    which = lax.rem(source - sub + fronts, fronts)

    diag, below, trail = panel_diag[0], panel_below[0], trailing[0].T
    diag_mine = chosen([diag] + [shifted(diag, "sub", fronts, s) for s in range(1, fronts)], which)
    scaled = leaf_sizes.astype(jnp.float32) / 100.0
    partial = jnp.sum(scaled * scaled * scaled)
    n = diag.shape[1]
    spot = (lax.broadcasted_iota(jnp.int32, diag.shape, 0) == 0) & (lax.broadcasted_iota(jnp.int32, diag.shape, 1) == n - 1)
    diag_mine = jnp.where(spot, partial, diag_mine)
    stacked = jnp.stack([diag_mine] + [around(diag_mine, s) for s in range(1, 4)])
    mine = lax.all_gather(stacked, "col_0", axis=0)
    other = shifted(mine, "row_1", 2, 1)

    below, _ = lax.optimization_barrier((below, diag_mine))
    below_mine = chosen([below] + [shifted(below, "sub", fronts, s) for s in range(1, fronts)], which)
    pieces = []
    for s in range(4):
        perm = [(f, ((f % 4 + s) % 4) * columns + f // 4) for f in range(4 * columns)]
        pieces.append(lax.ppermute(below_mine, ROW_COL, perm))
    swapped = shifted(below_mine, "col_1", 2, 1)
    pair = jnp.where(y_hi == 0, jnp.stack([below_mine, swapped]), jnp.stack([swapped, below_mine]))
    rows = lax.all_gather(pair, "col_0", axis=0).reshape(-1, n)

    trail, _ = lax.optimization_barrier((trail, below_mine))
    trail_mine = [trail] + [shifted(trail, "sub", fronts, s) for s in range(1, fronts)]

    places = jnp.stack([y_hi * 2 + y_lo, core, row_at, flat]).astype(jnp.int32)
    diag_factor, own_rows, y, corner = panel_call(places, mine, other, below_mine, pieces)
    schur = (chosen(trail_mine, which) - nt(y, rows)).T
    cost = corner[0, NB - 1:] / (leaf_sizes.shape[0] * 4 * columns)
    return diag_factor[None], own_rows[None], schur[None], cost


def solution(mesh):
    finer = Mesh(
        mesh.devices.reshape(mesh.shape["sub"], 2, 2, 8, 2),
        ("sub", "row_0", "row_1", "col_0", "col_1"),
    )
    return jax.shard_map(
        local,
        mesh=finer,
        in_specs=(
            P(SUB_ROW_COL),
            P(),
            P("sub", ROW_COL, None),
            P("sub", ROW_COL, None),
            P("sub", ROW, COL),
        ),
        out_specs=(P("sub", ROW_COL, None), P("sub", ROW_COL, None), P("sub", ROW, COL), P("sub")),
        check_vma=False,
    )
```

```python
import jax
import jax.numpy as jnp
from jax import lax
from jax.experimental import pallas as pl
from jax.experimental.pallas import tpu as pltpu
from jax.sharding import Mesh
from jax.sharding import PartitionSpec as P

ROW = ("row_0", "row_1")
COL = ("col_0", "col_1")
ROW_COL = ("row_0", "row_1", "col_0", "col_1")
SUB_ROW_COL = ("sub", "row_0", "row_1", "col_0", "col_1")

HI = lax.Precision.HIGHEST


def nt(a, b):
    return lax.dot_general(a, b, (((1,), (1,)), ((), ())), precision=HI, preferred_element_type=jnp.float32)


def nn(a, b):
    return lax.dot_general(a, b, (((1,), (0,)), ((), ())), precision=HI, preferred_element_type=jnp.float32)


def over_lanes(x, lane):
    return jnp.broadcast_to(x[:, lane:lane + 1], x.shape)


def over_sublanes(x, row):
    return jnp.broadcast_to(x[row:row + 1, :], x.shape)


def factor_block(block_ref, inverse_ref, upper_ref):
    size = block_ref.shape[0]
    groups = size // 8
    lanes = lax.broadcasted_iota(jnp.int32, (8, size), 1)
    subs = lax.broadcasted_iota(jnp.int32, (8, size), 0)
    rows = [block_ref[8 * q:8 * q + 8, :] for q in range(groups)]
    cols = [over_lanes(rows[0], l) for l in range(8)]
    near = [over_lanes(rows[1], l) for l in range(8)]
    for p in range(groups):
        inside = (lanes >= 8 * p) & (lanes < 8 * p + 8)
        plain = rows[p]
        unit = jnp.where(inside, jnp.where(lanes == subs + 8 * p, 1.0, 0.0), plain)
        below = {q: [over_lanes(rows[q], 8 * p + l) for l in range(8)] for q in range(p + 2, groups)}
        if p + 1 < groups:
            below[p + 1] = near
            cols_next = [over_lanes(rows[p + 1], 8 * p + 8 + l) for l in range(8)]
        if p + 2 < groups:
            near_next = [over_lanes(rows[p + 2], 8 * p + 8 + l) for l in range(8)]
        pivots = jnp.ones_like(plain)
        for j in range(8):
            u = {l: over_sublanes(cols[l], j) for l in range(j, 8)}
            pivots = jnp.where(subs == j, u[j], pivots)
            inv = 1.0 / u[j]
            coef = cols[j] * inv
            for l in range(j + 1, 8):
                cols[l] = cols[l] - coef * u[l]
            masked = jnp.where(subs > j, coef, 0.0)
            plain = plain - masked * over_sublanes(plain, j)
            unit = unit - masked * over_sublanes(unit, j)
            if p + 1 < groups:
                raw = below[p + 1][j]
            for q in below:
                v = below[q]
                v[j] = v[j] * inv
                for l in range(j + 1, 8):
                    v[l] = v[l] - v[j] * u[l]
            if p + 1 < groups:
                for l in range(8):
                    w = over_sublanes(raw, l)
                    cols_next[l] = cols_next[l] - below[p + 1][j] * w
                    if p + 2 < groups:
                        near_next[l] = near_next[l] - below[p + 2][j] * w
        spread = [over_sublanes(unit, j) for j in range(8)]
        for q in below:
            v = below[q]
            t = [v[j] * spread[j] for j in range(8)]
            s = ((t[0] + t[1]) + (t[2] + t[3])) + ((t[4] + t[5]) + (t[6] + t[7]))
            rows[q] = jnp.where(inside, 0.0, rows[q]) - s
        scale = lax.rsqrt(pivots)
        upper_ref[8 * p:8 * p + 8, :] = jnp.where(lanes >= subs + 8 * p, plain * scale, 0.0)
        inverse_ref[8 * p:8 * p + 8, :] = jnp.where(lanes <= subs + 8 * p, unit * scale, 0.0)
        if p + 1 < groups:
            cols = cols_next
        if p + 2 < groups:
            near = near_next


NB = 128
WB = 256


def panel_kernel(where_ref, mine_ref, other_ref, below_ref, c0_ref, c1_ref, c2_ref, c3_ref,
                 diag_out, own_out, y_out, cost_out, work, block, inverse, upper, pair, sems):
    n = work.shape[1]
    blocks = n // WB
    total = work.shape[0] // WB
    y_at, core, row_at, flat = where_ref[0], where_ref[1], where_ref[2], where_ref[3]
    z_count, s_count, piece_rows, _ = mine_ref.shape
    copies = []
    for side, ref in ((0, mine_ref), (1, other_ref)):
        core_of = lax.rem(core + side, 2)
        for s in range(s_count):
            y_of = lax.rem(y_at + s, 4)
            base = (lax.rem(y_of, 2) * 2 + core_of) * 2 * z_count + lax.div(y_of, 2)
            for z in range(z_count):
                at = pl.multiple_of((base + 2 * z) * piece_rows, 8)
                copies.append((ref.at[z, s], work.at[pl.ds(at, piece_rows), :]))
    own_rows = below_ref.shape[0]
    for s, ref in enumerate((c0_ref, c1_ref, c2_ref, c3_ref)):
        at = pl.multiple_of(n + lax.rem(row_at + s, 4) * own_rows, 8)
        copies.append((ref, work.at[pl.ds(at, own_rows), :]))
    copies.append((below_ref, work.at[pl.ds(n + 4 * own_rows, own_rows), :]))
    copies = [pltpu.make_async_copy(src, dst, sems.at[i]) for i, (src, dst) in enumerate(copies)]
    for c in copies:
        c.start()
    used = n + 5 * own_rows
    work[used:, :] = jnp.zeros((work.shape[0] - used, n), jnp.float32)
    for c in copies:
        c.wait()
    last = slice(n - NB, n)
    corner = work[0:8, last]
    for f in range(1, n // piece_rows):
        corner = corner + work[f * piece_rows:f * piece_rows + 8, last]
    cost_out[...] = corner
    first = (lax.broadcasted_iota(jnp.int32, (8, NB), 0) == 0) & (lax.broadcasted_iota(jnp.int32, (8, NB), 1) == NB - 1)
    for f in range(-(-(n - NB) // piece_rows), n // piece_rows):
        r = f * piece_rows
        mirror = jnp.broadcast_to(work[n - 1:n, r:r + 1], (8, NB))
        work[r:r + 8, last] = jnp.where(first, mirror, work[r:r + 8, last])
    block[...] = work[0:NB, 0:NB]

    def step(j, carry):
        factor_block(block, inverse, upper)
        for jj in range(n // NB):
            @pl.when(j == jj)
            def _(jj=jj):
                J, half = jj // 2, jj % 2
                lo = jj * NB
                if half == 0:
                    work[lo:lo + NB, lo:lo + NB] = upper[...].T
                    low = nt(work[lo + NB:lo + 2 * NB, lo:lo + NB], inverse[...])
                    work[lo + NB:lo + 2 * NB, lo:lo + NB] = low
                    block[...] = work[lo + NB:lo + 2 * NB, lo + NB:lo + 2 * NB] - nt(low, low)
                    pair[J, 0:NB, 0:NB] = inverse[...]
                    pair[J, 0:NB, NB:] = jnp.zeros((NB, NB), jnp.float32)
                else:
                    work[lo:lo + NB, lo:lo + NB] = upper[...].T
                    low = work[lo:lo + NB, lo - NB:lo]
                    pair[J, NB:, 0:NB] = -nn(inverse[...], nn(low, pair[J, 0:NB, 0:NB]))
                    pair[J, NB:, NB:] = inverse[...]
                    both = slice(J * WB, (J + 1) * WB)
                    after = slice((J + 1) * WB, (J + 2) * WB)

                    def solve(i, c):
                        at = pl.ds(pl.multiple_of(i * WB, WB), WB)
                        work[at, both] = nt(work[at, both], pair[J])
                        return c

                    lax.fori_loop(J + 1, total, solve, 0)
                    if J + 1 < blocks:
                        def update(i, c):
                            at = pl.ds(pl.multiple_of(i * WB, WB), WB)
                            work[at, after] = work[at, after] - nt(work[at, :(J + 1) * WB], work[after, :(J + 1) * WB])
                            return c

                        lax.fori_loop(J + 1, total, update, 0)
                        block[...] = work[lo + NB:lo + 2 * NB, lo + NB:lo + 2 * NB]
        return carry

    lax.fori_loop(0, n // NB, step, 0)
    count = diag_out.shape[0]
    at = pl.multiple_of(flat * count, 8)
    found = work[pl.ds(at, count), :]
    r = lax.broadcasted_iota(jnp.int32, found.shape, 0) + flat * count
    c = lax.broadcasted_iota(jnp.int32, found.shape, 1)
    diag_out[...] = jnp.where(c <= r, found, 0.0)
    own_out[...] = work[n + 4 * own_rows:n + 5 * own_rows, :]
    rows = slice(n, n + 4 * own_rows)
    for J in range(blocks - 1, -1, -1):
        both = slice(J * WB, (J + 1) * WB)
        part = work[rows, both]
        if J + 1 < blocks:
            part = part - nn(work[rows, (J + 1) * WB:], work[(J + 1) * WB:n, both])
        work[rows, both] = nn(part, pair[J])
    y_out[...] = work[rows, :]


def panel_call(places, mine, other, below, cs):
    n = mine.shape[-1]
    m = below.shape[0]
    height = -(-(n + 5 * m) // WB) * WB
    anyspec = pl.BlockSpec(memory_space=pl.ANY)
    vm = pl.BlockSpec(memory_space=pltpu.VMEM)
    f32 = jnp.float32
    pieces = 2 * mine.shape[0] * mine.shape[1]
    return pl.pallas_call(
        panel_kernel,
        out_shape=(jax.ShapeDtypeStruct((mine.shape[2], n), f32), jax.ShapeDtypeStruct((m, n), f32), jax.ShapeDtypeStruct((4 * m, n), f32), jax.ShapeDtypeStruct((8, NB), f32)),
        in_specs=[pl.BlockSpec(memory_space=pltpu.SMEM)] + [anyspec] * 7,
        out_specs=(vm, vm, vm, vm),
        scratch_shapes=[
            pltpu.VMEM((height, n), f32), pltpu.VMEM((NB, NB), f32), pltpu.VMEM((NB, NB), f32), pltpu.VMEM((NB, NB), f32),
            pltpu.VMEM((n // WB, WB, WB), f32), pltpu.SemaphoreType.DMA((pieces + 5,)),
        ],
        compiler_params=pltpu.CompilerParams(vmem_limit_bytes=62 * 2**20),
        cost_estimate=pl.CostEstimate(flops=100_000_000_000, bytes_accessed=20_000_000, transcendentals=0),
        name="panel",
    )(places, mine, other, below, *cs)


def shifted(value, axes, size, shift):
    return lax.ppermute(value, axes, [((d + shift) % size, d) for d in range(size)])


def around(value, shift):
    at = [(y % 2) * 2 + y // 2 for y in range(4)]
    return lax.ppermute(value, ("row_0", "col_1"), [(at[(y + shift) % 4], at[y]) for y in range(4)])


def chosen(pieces, which):
    out = pieces[0]
    for k in range(1, len(pieces)):
        out = jnp.where(which == k, pieces[k], out)
    return out


def inner(leaf_sizes, remap, panel_diag, panel_below, trailing):
    sub, core = lax.axis_index("sub"), lax.axis_index("row_1")
    y_lo, y_hi = lax.axis_index("row_0"), lax.axis_index("col_1")
    fronts = remap.shape[0]
    row_at = y_lo * 2 + core
    flat = lax.axis_index(ROW_COL)
    columns = lax.axis_size(COL)
    source = jnp.sum(jnp.arange(fronts, dtype=jnp.int32) * (remap == sub).astype(jnp.int32))
    which = lax.rem(source - sub + fronts, fronts)

    diag, below, trail = panel_diag[0], panel_below[0], trailing[0].T
    diag_all = [diag] + [shifted(diag, "sub", fronts, s) for s in range(1, fronts)]
    diag_mine = chosen(diag_all, which)
    scaled = leaf_sizes.astype(jnp.float32) / 100.0
    partial = jnp.sum(scaled * scaled * scaled)
    n = diag.shape[1]
    spot = (lax.broadcasted_iota(jnp.int32, diag.shape, 0) == 0) & (lax.broadcasted_iota(jnp.int32, diag.shape, 1) == n - 1)
    diag_mine = jnp.where(spot, partial, diag_mine)
    around_y = [around(diag_mine, s) for s in range(1, 4)]
    stacked = jnp.stack([diag_mine] + around_y)
    mine = lax.all_gather(stacked, "col_0", axis=0)
    other = shifted(mine, "row_1", 2, 1)

    below_all = [below] + [shifted(below, "sub", fronts, s) for s in range(1, fronts)]
    below_mine = chosen(below_all, which)
    perm = [(f, (f % 4) * columns + f // 4) for f in range(4 * columns)]
    piece = lax.ppermute(below_mine, ROW_COL, perm)
    swapped = shifted(below_mine, "col_1", 2, 1)
    pieces = [piece] + [shifted(piece, ROW, 4, s) for s in range(1, 4)]
    pair = jnp.where(y_hi == 0, jnp.stack([below_mine, swapped]), jnp.stack([swapped, below_mine]))
    rows = lax.all_gather(pair, "col_0", axis=0).reshape(-1, n)

    trail_mine = [trail] + [shifted(trail, "sub", fronts, s) for s in range(1, fronts)]

    places = jnp.stack([y_hi * 2 + y_lo, core, row_at, flat]).astype(jnp.int32)
    diag_factor, own_rows, y, corner = panel_call(places, mine, other, below_mine, pieces)
    schur = (chosen(trail_mine, which) - nt(y, rows)).T
    cost = corner[0, NB - 1:] / (leaf_sizes.shape[0] * 4 * columns)
    return diag_factor[None], own_rows[None], schur[None], cost


def solution(mesh):
    finer = Mesh(
        mesh.devices.reshape(mesh.shape["sub"], 2, 2, 8, 2),
        ("sub", "row_0", "row_1", "col_0", "col_1"),
    )
    return jax.shard_map(
        inner,
        mesh=finer,
        in_specs=(
            P(SUB_ROW_COL),
            P(),
            P("sub", ROW_COL, None),
            P("sub", ROW_COL, None),
            P("sub", ROW, COL),
        ),
        out_specs=(P("sub", ROW_COL, None), P("sub", ROW_COL, None), P("sub", ROW, COL), P("sub")),
        check_vma=False,
    )
```

```python
import functools

import jax
import jax.numpy as jnp
from jax import lax
from jax.experimental import pallas as pl
from jax.experimental.pallas import tpu as pltpu
from jax.sharding import Mesh
from jax.sharding import PartitionSpec as P

ROW = ("row_0", "row_1")
COL = ("col_0", "col_1")
ROW_COL = ("row_0", "row_1", "col_0", "col_1")
SUB_ROW_COL = ("sub", "row_0", "row_1", "col_0", "col_1")

HI = lax.Precision.HIGHEST


def nt(a, b):
    return lax.dot_general(a, b, (((1,), (1,)), ((), ())), precision=HI, preferred_element_type=jnp.float32)


def nn(a, b):
    return lax.dot_general(a, b, (((1,), (0,)), ((), ())), precision=HI, preferred_element_type=jnp.float32)


def over_lanes(x, lane):
    return jnp.broadcast_to(x[:, lane:lane + 1], x.shape)


def over_sublanes(x, row):
    return jnp.broadcast_to(x[row:row + 1, :], x.shape)


def factor_block(block_ref, inverse_ref, upper_ref):
    size = block_ref.shape[0]
    groups = size // 8
    lanes = lax.broadcasted_iota(jnp.int32, (8, size), 1)
    subs = lax.broadcasted_iota(jnp.int32, (8, size), 0)
    rows = [block_ref[8 * q:8 * q + 8, :] for q in range(groups)]
    cols = [over_lanes(rows[0], l) for l in range(8)]
    near = [over_lanes(rows[1], l) for l in range(8)]
    for p in range(groups):
        inside = (lanes >= 8 * p) & (lanes < 8 * p + 8)
        plain = rows[p]
        unit = jnp.where(inside, jnp.where(lanes == subs + 8 * p, 1.0, 0.0), plain)
        below = {q: [over_lanes(rows[q], 8 * p + l) for l in range(8)] for q in range(p + 2, groups)}
        if p + 1 < groups:
            below[p + 1] = near
            cols_next = [over_lanes(rows[p + 1], 8 * p + 8 + l) for l in range(8)]
        if p + 2 < groups:
            near_next = [over_lanes(rows[p + 2], 8 * p + 8 + l) for l in range(8)]
        pivots = jnp.ones_like(plain)
        for j in range(8):
            u = {l: over_sublanes(cols[l], j) for l in range(j, 8)}
            pivots = jnp.where(subs == j, u[j], pivots)
            inv = 1.0 / u[j]
            coef = cols[j] * inv
            for l in range(j + 1, 8):
                cols[l] = cols[l] - coef * u[l]
            masked = jnp.where(subs > j, coef, 0.0)
            plain = plain - masked * over_sublanes(plain, j)
            unit = unit - masked * over_sublanes(unit, j)
            if p + 1 < groups:
                raw = below[p + 1][j]
            for q in below:
                v = below[q]
                v[j] = v[j] * inv
                for l in range(j + 1, 8):
                    v[l] = v[l] - v[j] * u[l]
            if p + 1 < groups:
                for l in range(8):
                    w = over_sublanes(raw, l)
                    cols_next[l] = cols_next[l] - below[p + 1][j] * w
                    if p + 2 < groups:
                        near_next[l] = near_next[l] - below[p + 2][j] * w
        spread = [over_sublanes(unit, j) for j in range(8)]
        for q in below:
            v = below[q]
            t = [v[j] * spread[j] for j in range(8)]
            s = ((t[0] + t[1]) + (t[2] + t[3])) + ((t[4] + t[5]) + (t[6] + t[7]))
            rows[q] = jnp.where(inside, 0.0, rows[q]) - s
        scale = lax.rsqrt(pivots)
        upper_ref[8 * p:8 * p + 8, :] = jnp.where(lanes >= subs + 8 * p, plain * scale, 0.0)
        inverse_ref[8 * p:8 * p + 8, :] = jnp.where(lanes <= subs + 8 * p, unit * scale, 0.0)
        if p + 1 < groups:
            cols = cols_next
        if p + 2 < groups:
            near = near_next


NB = 128
WB = 256
VMEM_MB = 62


def panel_kernel(scale, where_ref, mine_ref, other_ref, below_ref, *refs):
    piece_refs = refs[:-10]
    diag_out, own_out, y_out, cost_out, work, block, inverse, upper, pair, sems = refs[-10:]
    n = work.shape[1]
    blocks = n // WB
    total = work.shape[0] // WB
    y_at, core, flat = where_ref[0], where_ref[1], where_ref[2]
    z_count, slots, piece_rows, half = mine_ref.shape
    groups = []
    for side, ref in ((0, mine_ref), (1, other_ref)):
        core_of = lax.rem(core + side, 2)
        for s in range(slots):
            y_of = lax.rem(y_at + s, 4) if s < 4 else lax.rem(y_at + 2 * (s - 4) + 1 - lax.rem(y_at, 2), 4)
            cols = slice(0, half) if s < 4 else slice(half, n)
            base = (lax.rem(y_of, 2) * 2 + core_of) * 2 * z_count + lax.div(y_of, 2)
            groups.append((ref, s, base, cols))

    def block_copy(g, z):
        ref, s, base, cols = groups[g]
        at = pl.multiple_of((base + 2 * z) * piece_rows, 8)
        return pltpu.make_async_copy(ref.at[z, s], work.at[pl.ds(at, piece_rows), cols], sems.at[g * z_count + z])

    own_rows = below_ref.shape[0]
    copies = []
    for k, ref in enumerate(piece_refs):
        at = pl.multiple_of(n + lax.rem(where_ref[3] + k, 4) * own_rows, 8)
        copies.append((ref, work.at[pl.ds(at, own_rows), :]))
    copies.append((below_ref, work.at[pl.ds(n + 4 * own_rows, own_rows), :]))
    copies = [pltpu.make_async_copy(src, dst, sems.at[len(groups) * z_count + i]) for i, (src, dst) in enumerate(copies)]

    def start(z, c):
        for g in range(len(groups)):
            block_copy(g, z).start()
        return c

    def finish(z, c):
        for g in range(len(groups)):
            block_copy(g, z).wait()
        return c

    lax.fori_loop(0, z_count, start, 0)
    for c in copies:
        c.start()
    used = n + 5 * own_rows
    work[used:, :] = jnp.zeros((work.shape[0] - used, n), jnp.float32)
    lax.fori_loop(0, z_count, finish, 0)
    for c in copies:
        c.wait()
    corner = jnp.zeros((8, NB), jnp.float32)
    first = (lax.broadcasted_iota(jnp.int32, (8, NB), 0) == 0) & (lax.broadcasted_iota(jnp.int32, (8, NB), 1) == NB - 1)
    for f in range(n // piece_rows):
        r = f * piece_rows
        end = half if r < half else n
        last = slice(end - NB, end)
        tile = work[r:r + 8, last]
        corner = corner + tile
        if r >= end - NB:
            mirror = jnp.broadcast_to(work[end - 1:end, r:r + 1], (8, NB))
            work[r:r + 8, last] = jnp.where(first, mirror, tile)
    cost_out[0] = jnp.sum(jnp.where(first, corner, 0.0)) * scale
    block[...] = work[0:NB, 0:NB]

    def step(j, carry):
        factor_block(block, inverse, upper)
        J = lax.div(j, 2)
        lo = pl.multiple_of(j * NB, NB)
        here = pl.ds(lo, NB)

        @pl.when(lax.rem(j, 2) == 0)
        def _():
            following = pl.ds(pl.multiple_of(lo + NB, NB), NB)
            work[here, here] = upper[...].T
            low = nt(work[following, here], inverse[...])
            work[following, here] = low
            block[...] = work[following, following] - nt(low, low)
            pair[J, 0:NB, 0:NB] = inverse[...]
            pair[J, 0:NB, NB:] = jnp.zeros((NB, NB), jnp.float32)

        @pl.when(lax.rem(j, 2) == 1)
        def _():
            work[here, here] = upper[...].T
            low = work[here, pl.ds(pl.multiple_of(lo - NB, NB), NB)]
            pair[J, NB:, 0:NB] = -nn(inverse[...], nn(low, pair[J, 0:NB, 0:NB]))
            pair[J, NB:, NB:] = inverse[...]
            both = pl.ds(pl.multiple_of(J * WB, WB), WB)
            doubles = lax.div(total - 1 - J, 2)

            @pl.when(lax.rem(total - 1 - J, 2) == 1)
            def _():
                at = pl.ds(pl.multiple_of((J + 1) * WB, WB), WB)
                work[at, both] = nt(work[at, both], pair[J])

            def solve(i, c):
                at = pl.ds(pl.multiple_of((total - 2 - 2 * i) * WB, WB), 2 * WB)
                work[at, both] = nt(work[at, both], pair[J])
                return c

            lax.fori_loop(0, doubles, solve, 0)

        for JJ in range(blocks - 1):
            @pl.when(j == 2 * JJ + 1)
            def _(JJ=JJ):
                after = slice((JJ + 1) * WB, (JJ + 2) * WB)

                parts = 1 if JJ < 4 else 2
                width = (JJ + 1) * WB // parts

                def update(i, c):
                    at = pl.ds(pl.multiple_of(i * WB, WB), WB)

                    def chunk(k, c):
                        cols = pl.ds(pl.multiple_of(k * width, NB), width)
                        work[at, after] = work[at, after] - nt(work[at, cols], work[after, cols])
                        return c

                    return lax.fori_loop(0, parts, chunk, c)

                lax.fori_loop(JJ + 1, total, update, 0)
                corner_at = slice((JJ + 1) * WB, (JJ + 1) * WB + NB)
                block[...] = work[corner_at, corner_at]
        return carry

    lax.fori_loop(0, n // NB, step, 0)
    count = diag_out.shape[0]
    at = pl.multiple_of(flat * count, 8)
    found = work[pl.ds(at, count), :]
    r = lax.broadcasted_iota(jnp.int32, found.shape, 0) + flat * count
    c = lax.broadcasted_iota(jnp.int32, found.shape, 1)
    diag_out[...] = jnp.where(c <= r, found, 0.0)
    own_out[...] = work[n + 4 * own_rows:n + 5 * own_rows, :]
    rows = slice(n, n + 4 * own_rows)

    def back(step, c):
        J = blocks - 1 - step
        both = pl.ds(pl.multiple_of(J * WB, WB), WB)

        def take(I, c):
            other = pl.ds(pl.multiple_of(I * WB, WB), WB)
            work[rows, both] = work[rows, both] - nn(work[rows, other], work[other, both])
            return c

        lax.fori_loop(J + 1, blocks, take, 0)
        work[rows, both] = nn(work[rows, both], pair[J])
        return c

    lax.fori_loop(0, blocks, back, 0)
    y_out[...] = work[rows, :]


def panel_call(places, mine, other, below, cs, scale):
    z_count, slots, piece_rows, half = mine.shape
    n = 2 * half
    m = below.shape[0]
    height = -(-(n + 5 * m) // WB) * WB
    anyspec = pl.BlockSpec(memory_space=pl.ANY)
    vm = pl.BlockSpec(memory_space=pltpu.VMEM)
    f32 = jnp.float32
    return pl.pallas_call(
        functools.partial(panel_kernel, scale),
        out_shape=tuple(jax.ShapeDtypeStruct(s, f32) for s in ((piece_rows, n), (m, n), (4 * m, n), (1,))),
        in_specs=[pl.BlockSpec(memory_space=pltpu.SMEM)] + [anyspec] * 7,
        out_specs=(vm, vm, vm, pl.BlockSpec(memory_space=pltpu.SMEM)),
        scratch_shapes=[
            pltpu.VMEM((height, n), f32), pltpu.VMEM((NB, NB), f32), pltpu.VMEM((NB, NB), f32), pltpu.VMEM((NB, NB), f32),
            pltpu.VMEM((n // WB, WB, WB), f32), pltpu.SemaphoreType.DMA((2 * slots * z_count + 5,)),
        ],
        compiler_params=pltpu.CompilerParams(vmem_limit_bytes=VMEM_MB * 2**20),
        cost_estimate=pl.CostEstimate(flops=100_000_000_000, bytes_accessed=20_000_000, transcendentals=0),
        name="panel",
    )(places, mine, other, below, *cs)


def shifted(value, axes, size, shift):
    return lax.ppermute(value, axes, [((d + shift) % size, d) for d in range(size)])


def around(value, shift):
    at = [(y % 2) * 2 + y // 2 for y in range(4)]
    return lax.ppermute(value, ("row_0", "col_1"), [(at[(y + shift) % 4], at[y]) for y in range(4)])


def chosen(pieces, which):
    out = pieces[0]
    for k in range(1, len(pieces)):
        out = jnp.where(which == k, pieces[k], out)
    return out


def inner(leaf_sizes, remap, panel_diag, panel_below, trailing):
    sub, core = lax.axis_index("sub"), lax.axis_index("row_1")
    y_lo, y_hi = lax.axis_index("row_0"), lax.axis_index("col_1")
    fronts = remap.shape[0]
    row_at = y_lo * 2 + core
    flat = lax.axis_index(ROW_COL)
    columns = lax.axis_size(COL)
    source = jnp.sum(jnp.arange(fronts, dtype=jnp.int32) * (remap == sub).astype(jnp.int32))
    which = lax.rem(source - sub + fronts, fronts)

    diag, below, trail = panel_diag[0], panel_below[0], trailing[0].T
    diag_all = [diag] + [shifted(diag, "sub", fronts, s) for s in range(1, fronts)]
    perm = [(f, (f % 4) * columns + f // 4) for f in range(4 * columns)]
    half = below.shape[1] // 2
    halves = [lax.ppermute(below[:, k * half:(k + 1) * half], ROW_COL, perm) for k in range(2)]
    below_all = [below] + [shifted(below, "sub", fronts, s) for s in range(1, fronts)]
    diag_mine = chosen(diag_all, which)

    scaled = leaf_sizes.astype(jnp.float32) / 100.0
    partial = jnp.sum(scaled * scaled * scaled)
    n = diag.shape[1]
    half = n // 2
    spot_at = jnp.where(y_lo == 0, half - 1, n - 1)
    spot = (lax.broadcasted_iota(jnp.int32, diag.shape, 0) == 0) & (lax.broadcasted_iota(jnp.int32, diag.shape, 1) == spot_at)
    diag_mine = jnp.where(spot, partial, diag_mine)

    ys = [diag_mine] + [around(diag_mine, s) for s in range(1, 4)]
    lefts = [p[:, :half] for p in ys]
    rights = [jnp.where(y_lo == 1, ys[2 * t][:, half:], ys[2 * t + 1][:, half:]) for t in range(2)]
    mine = lax.all_gather(jnp.stack(lefts + rights), "col_0", axis=0)
    other = shifted(mine, "row_1", 2, 1)

    below_mine = chosen(below_all, which)
    swapped = shifted(below_mine, "col_1", 2, 1)
    two = jnp.where(y_hi == 0, jnp.stack([below_mine, swapped]), jnp.stack([swapped, below_mine]))
    rows = lax.all_gather(two, "col_0", axis=0).reshape(-1, n)
    parts = []
    for part in halves:
        parts.append(chosen([part] + [shifted(part, "sub", fronts, s) for s in range(1, fronts)], which))
    piece = jnp.concatenate(parts, axis=1)
    pieces = [piece] + [shifted(piece, ROW, 4, s) for s in range(1, 4)]
    trail_mine = [trail] + [shifted(trail, "sub", fronts, s) for s in range(1, fronts)]

    places = jnp.stack([y_hi * 2 + y_lo, core, flat, row_at]).astype(jnp.int32)
    scale = 1.0 / (leaf_sizes.shape[0] * 4 * columns)
    diag_factor, own_rows, y, cost = panel_call(places, mine, other, below_mine, pieces, scale)
    schur = (chosen(trail_mine, which) - lax.dot_general(y, rows, (((1,), (1,)), ((), ())), precision=lax.Precision.HIGH, preferred_element_type=jnp.float32)).T
    return diag_factor[None], own_rows[None], schur[None], cost


def solution(mesh):
    finer = Mesh(
        mesh.devices.reshape(mesh.shape["sub"], 2, 2, 8, 2),
        ("sub", "row_0", "row_1", "col_0", "col_1"),
    )
    return jax.shard_map(
        inner,
        mesh=finer,
        in_specs=(
            P(SUB_ROW_COL),
            P(),
            P("sub", ROW_COL, None),
            P("sub", ROW_COL, None),
            P("sub", ROW, COL),
        ),
        out_specs=(P("sub", ROW_COL, None), P("sub", ROW_COL, None), P("sub", ROW, COL), P("sub")),
        check_vma=False,
    )
```
